32 devices in a mesh: dp: 2 (over z, core), tp: 16 (over x, y).
Axes of the slice: x: 4, y: 4, z: 1, core: 2. Of those that a mesh axis runs over, the one named last changes fastest.
The devices are a block of a 4x4x8 slice.
Arguments:
- x: bfloat16 [128, 4096], P('dp'), parts along dimension 0
- k_cache: bfloat16 [128, 2048, 64, 64], P('dp', None, 'tp'), parts along dimension 0
- v_cache: bfloat16 [128, 2048, 64, 64], P('dp', None, 'tp'), parts along dimension 0
- gain_a: bfloat16 [4096], replicated
- wq: bfloat16 [4096, 4096], P(None, 'tp')
- wo: bfloat16 [4096, 4096], P('tp')
- gain_m: bfloat16 [4096], replicated
- w_gate: bfloat16 [4096, 10240], P(None, 'tp')
- w_up: bfloat16 [4096, 10240], P(None, 'tp')
- w_down: bfloat16 [10240, 4096], P('tp')
Outputs:
- output: bfloat16 [128, 4096], P('dp'), parts along dimension 0
There are 2 independent parts. The reference program is written for one: setup_inputs(seed, part) draws one part's arguments, and reference() takes and returns one part's arrays. A program takes and returns all parts, laid end to end along the dimension named above; an argument that names none is the same for every part.
All inputs are finite; a program needn't handle non-finite values.
Results may differ from the reference program's by a relative error of at most 0.017.
Values are sent between devices in bfloat16 or wider.
A program may use at most 768 MiB of HBM per device.

```python
import jax
import jax.numpy as jnp
from jax import lax

BATCH = 64
CACHE = 2048
D = 4096
HEADS = 64
KV_HEADS = 64
HEAD = 64
FF = 10240
THETA = 10000


def setup_inputs(seed: int = 0, part: int = 0) -> dict:
    kx, kc, kw, kn, kq, ko, km, kg, ku, kd = jax.random.split(jax.random.key(seed), 10)
    kx, kc, kw = (jax.random.fold_in(k, part) for k in (kx, kc, kw))

    def weights(key, rows, columns):
        return jax.random.normal(key, (rows, columns), jnp.float32) * rows**-0.5

    drawn = {
        "x": jax.random.normal(kx, (BATCH, D), jnp.float32),
        "k_cache": 2 * jax.random.normal(kc, (BATCH, CACHE, KV_HEADS, HEAD), jnp.float32),
        "v_cache": 4 * jax.random.normal(kw, (BATCH, CACHE, KV_HEADS, HEAD), jnp.float32),
        "gain_a": 1 + 0.1 * jax.random.normal(kn, (D,), jnp.float32),
        "wq": 2 * weights(kq, D, HEADS * HEAD),
        "wo": weights(ko, HEADS * HEAD, D),
        "gain_m": 1 + 0.1 * jax.random.normal(km, (D,), jnp.float32),
        "w_gate": weights(kg, D, FF),
        "w_up": weights(ku, D, FF),
        "w_down": 2 * weights(kd, FF, D),
    }
    return {k: v.astype(jnp.bfloat16) for k, v in drawn.items()}


def normed(x, gain):
    wide = x.astype(jnp.float32)
    scale = lax.rsqrt(jnp.mean(wide * wide, -1, keepdims=True) + 1e-6)
    return (wide * scale * gain.astype(jnp.float32)).astype(jnp.bfloat16)


def turned(t, place, theta):
    half = t.shape[-1] // 2
    angle = place.astype(jnp.float32)[:, None] * theta ** (-jnp.arange(half, dtype=jnp.float32) / half)
    cos, sin = jnp.cos(angle)[:, None], jnp.sin(angle)[:, None]
    a, b = t[..., :half].astype(jnp.float32), t[..., half:].astype(jnp.float32)
    return jnp.concatenate([a * cos - b * sin, b * cos + a * sin], -1).astype(jnp.bfloat16)


def matmul(a, w):
    return jnp.dot(a, w, preferred_element_type=jnp.float32).astype(jnp.bfloat16)


def einsum(form, a, b):
    return jnp.einsum(form, a.astype(jnp.float32), b.astype(jnp.float32))


def seen_by(a, wq, k_cache, v_cache, head, theta):
    batch, cache, kv_heads = k_cache.shape[:3]
    place = jnp.full((batch,), cache - 1)
    q = turned(matmul(a, wq).reshape(batch, -1, head), place, theta).reshape(batch, kv_heads, -1, head)
    scores = einsum("bgsd,bugd->bgsu", q, k_cache) * head**-0.5
    weights = jax.nn.softmax(scores, -1).astype(jnp.bfloat16)
    return einsum("bgsu,bugd->bgsd", weights, v_cache).astype(jnp.bfloat16).reshape(batch, -1)


def hidden_of(b, w_gate, w_up):
    gate = jnp.dot(b, w_gate, preferred_element_type=jnp.float32)
    up = jnp.dot(b, w_up, preferred_element_type=jnp.float32)
    return (jax.nn.silu(gate) * up).astype(jnp.bfloat16)


def reference(x, k_cache, v_cache, gain_a, wq, wo, gain_m, w_gate, w_up, w_down):
    seen = seen_by(normed(x, gain_a), wq, k_cache, v_cache, HEAD, THETA)
    h = (x.astype(jnp.float32) + jnp.dot(seen, wo, preferred_element_type=jnp.float32)).astype(jnp.bfloat16)
    hidden = hidden_of(normed(h, gain_m), w_gate, w_up)
    return (h.astype(jnp.float32) + jnp.dot(hidden, w_down, preferred_element_type=jnp.float32)).astype(jnp.bfloat16)
```

```python
import functools

import jax
import jax.numpy as jnp
from jax import lax
from jax.experimental import pallas as pl
from jax.experimental.pallas import tpu as pltpu
from jax.sharding import PartitionSpec as P

HEAD = 64
THETA = 10000


def normed(x, gain):
    wide = x.astype(jnp.float32)
    scale = lax.rsqrt(jnp.mean(wide * wide, -1, keepdims=True) + 1e-6)
    return (wide * scale * gain.astype(jnp.float32)).astype(jnp.bfloat16)


def turned(t, place, theta):
    half = t.shape[-1] // 2
    angle = place.astype(jnp.float32)[:, None] * theta ** (-jnp.arange(half, dtype=jnp.float32) / half)
    cos, sin = jnp.cos(angle)[:, None], jnp.sin(angle)[:, None]
    a, b = t[..., :half].astype(jnp.float32), t[..., half:].astype(jnp.float32)
    return jnp.concatenate([a * cos - b * sin, b * cos + a * sin], -1).astype(jnp.bfloat16)


def matmul(a, w):
    return jnp.dot(a, w, preferred_element_type=jnp.float32).astype(jnp.bfloat16)


def einsum(form, a, b):
    return jnp.einsum(form, a.astype(jnp.float32), b.astype(jnp.float32))


def seen_by(a, wq, k_cache, v_cache, head, theta):
    batch, cache, kv_heads = k_cache.shape[:3]
    place = jnp.full((batch,), cache - 1)
    q = turned(matmul(a, wq).reshape(batch, -1, head), place, theta).reshape(batch, kv_heads, -1, head)
    scores = einsum("bgsd,bugd->bgsu", q, k_cache) * head**-0.5
    weights = jax.nn.softmax(scores, -1).astype(jnp.bfloat16)
    return einsum("bgsu,bugd->bgsd", weights, v_cache).astype(jnp.bfloat16).reshape(batch, -1)


def hidden_of(b, w_gate, w_up):
    gate = jnp.dot(b, w_gate, preferred_element_type=jnp.float32)
    up = jnp.dot(b, w_up, preferred_element_type=jnp.float32)
    return (jax.nn.silu(gate) * up).astype(jnp.bfloat16)


def sum_kernel(n, t_ref, term_ref, out_ref, got, send_sem, recv_sem, send2_sem, recv2_sem):
    me = lax.axis_index("tp")
    rows, width = t_ref.shape
    cols = width // n

    def block(p):
        return pl.ds(pl.multiple_of(p * cols, cols), cols)

    barrier = pltpu.get_barrier_semaphore()
    for k in range(1, n):
        pl.semaphore_signal(barrier, inc=1, device_id={"tp": lax.rem(me + k, n)})
    pl.semaphore_wait(barrier, n - 1)

    sends = []
    for k in range(1, n):
        p = lax.rem(me + k, n)
        copy = pltpu.make_async_remote_copy(
            src_ref=term_ref.at[:, block(p)],
            dst_ref=got.at[k - 1],
            send_sem=send_sem.at[k - 1],
            recv_sem=recv_sem.at[k - 1],
            device_id={"tp": p},
        )
        copy.start()
        sends.append(copy)
    total = t_ref[:, block(me)].astype(jnp.float32) + term_ref[:, block(me)].astype(jnp.float32)
    for k in range(1, n):
        sends[k - 1].wait_recv()
        total += got[k - 1].astype(jnp.float32)
    out_ref[:, block(me)] = total.astype(jnp.bfloat16)
    shares = []
    for k in range(1, n):
        p = lax.rem(me + k, n)
        copy = pltpu.make_async_remote_copy(
            src_ref=out_ref.at[:, block(me)],
            dst_ref=out_ref.at[:, block(me)],
            send_sem=send2_sem.at[k - 1],
            recv_sem=recv2_sem.at[k - 1],
            device_id={"tp": p},
        )
        copy.start()
        shares.append(copy)
    for copy in shares:
        copy.wait_recv()
    for copy in sends + shares:
        copy.wait_send()


def solution(mesh):
    n = mesh.shape["tp"]

    def added(t, term):
        rows, width = t.shape
        vmem = pl.BlockSpec(memory_space=pltpu.VMEM)
        return pl.pallas_call(
            functools.partial(sum_kernel, n),
            out_shape=jax.ShapeDtypeStruct(t.shape, jnp.bfloat16),
            in_specs=[vmem, vmem],
            out_specs=vmem,
            scratch_shapes=[pltpu.VMEM((n - 1, rows, width // n), jnp.bfloat16)]
            + [pltpu.SemaphoreType.DMA((n - 1,))] * 4,
            compiler_params=pltpu.CompilerParams(collective_id=0, has_side_effects=True),
            name="added",
        )(t, term.astype(jnp.bfloat16))

    def step(x, k_cache, v_cache, gain_a, wq, wo, gain_m, w_gate, w_up, w_down):
        seen = seen_by(normed(x, gain_a), wq, k_cache, v_cache, HEAD, THETA)
        h = added(x, jnp.dot(seen, wo, preferred_element_type=jnp.float32))
        return added(h, jnp.dot(hidden_of(normed(h, gain_m), w_gate, w_up), w_down, preferred_element_type=jnp.float32))

    states, cache, columns, rows_of = P("dp", None), P("dp", None, "tp", None), P(None, "tp"), P("tp", None)
    return jax.shard_map(
        step,
        mesh=mesh,
        in_specs=(states, cache, cache, P(None), columns, rows_of, P(None), columns, columns, rows_of),
        out_specs=states,
        check_vma=False,
    )
```

```python
import functools

import jax
import jax.numpy as jnp
import numpy as np
from jax import lax
from jax.experimental import pallas as pl
from jax.experimental.pallas import tpu as pltpu
from jax.sharding import PartitionSpec as P

HEAD = 64
THETA = 10000
GROUP = 4
CHUNK = 16
SLOTS = 3

F32, BF16 = jnp.float32, jnp.bfloat16


def iota(shape, axis):
    return lax.broadcasted_iota(jnp.int32, shape, axis)


def layer_kernel(n, dims, x_hbm, k_hbm, v_hbm, gain_a, wq_hbm, wo_hbm, gain_m, wg_hbm, wu_hbm, wd_hbm, turn, out,
                 x, a, wq, wo, wgu, wd, kbuf, vbuf, qx, seen, term, h, got, term2, got2,
                 in_sem, k_sem, v_sem, send_sem, rs_sem, ag_sem, rs2_sem, ag2_sem):
    batch, width, heads, cache, hidden = dims
    mine = heads * HEAD
    cols = width // n
    chunks, groups = batch // CHUNK, batch // GROUP
    per = groups // chunks
    me = lax.axis_index("tp")

    def block(p):
        return pl.ds(pl.multiple_of(p * cols, cols), cols)

    def rows(c):
        return pl.ds(pl.multiple_of(c * CHUNK, CHUNK), CHUNK)

    def peer(k):
        return lax.rem(me + k, n)

    def take(i, src, dst):
        return pltpu.make_async_copy(src, dst, in_sem.at[i])

    take_x, take_wq, take_wo = take(0, x_hbm, x), take(1, wq_hbm, wq), take(2, wo_hbm, wo)
    take_wg = take(3, wg_hbm, wgu.at[:, pl.ds(0, hidden)])
    take_wu = take(4, wu_hbm, wgu.at[:, pl.ds(hidden, hidden)])
    take_wd = take(5, wd_hbm, wd)

    def take_k(g):
        s = lax.rem(g, SLOTS)
        return pltpu.make_async_copy(k_hbm.at[pl.ds(g * GROUP, GROUP)], kbuf.at[s], k_sem.at[s])

    def take_v(g):
        s = lax.rem(g, SLOTS)
        return pltpu.make_async_copy(v_hbm.at[pl.ds(g * GROUP, GROUP)], vbuf.at[s], v_sem.at[s])

    take_x.start()
    take_wq.start()
    for g in range(SLOTS):
        take_k(g).start()
        take_v(g).start()
        if g == 0:
            take_wo.start()

    barrier = pltpu.get_barrier_semaphore()
    for k in range(1, n):
        pl.semaphore_signal(barrier, inc=1, device_id={"tp": peer(k)})

    def all_arrived(sem):
        pltpu.make_async_copy(got.at[0], got.at[0], sem).wait()

    def scatter(c, src, dst, sem):
        for k in range(1, n):
            pltpu.make_async_remote_copy(
                src_ref=src.at[rows(c), block(peer(k))],
                dst_ref=dst.at[c, k - 1],
                send_sem=send_sem,
                recv_sem=sem.at[c],
                device_id={"tp": peer(k)},
            ).start()

    def share(c, ref, sem):
        for k in range(1, n):
            pltpu.make_async_remote_copy(
                src_ref=ref.at[rows(c), block(me)],
                dst_ref=ref.at[rows(c), block(me)],
                send_sem=send_sem,
                recv_sem=sem.at[c],
                device_id={"tp": peer(k)},
            ).start()

    def finish(c, base, own, came, dst):
        total = base[rows(c), block(me)].astype(F32) + own[rows(c), block(me)].astype(F32)
        for k in range(n - 1):
            total += came[c, k].astype(F32)
        dst[rows(c), block(me)] = total.astype(BF16)

    def norm(c, src, gain, dst):
        wide = src[rows(c), :].astype(F32)
        scale = lax.rsqrt(jnp.mean(wide * wide, -1, keepdims=True) + 1e-6)
        dst[rows(c), :] = (wide * scale * gain[...].astype(F32)).astype(BF16)

    def each(count, body):
        lax.fori_loop(0, count, lambda i, _: (body(i), None)[1], None)

    take_x.wait()
    each(chunks, lambda c: norm(c, x, gain_a, a))
    take_wq.wait()
    q = jnp.dot(a[...], wq[...], preferred_element_type=F32).astype(BF16).astype(F32)
    low = lax.rem(iota(q.shape, 1), HEAD) < HEAD // 2
    other = jnp.where(low, pltpu.roll(q, mine - HEAD // 2, 1), pltpu.roll(q, HEAD // 2, 1))
    q = (q * turn[0:1, :] + other * turn[1:2, :]).astype(BF16)
    spread = (iota((batch * heads, batch), 0) // heads == iota((batch * heads, batch), 1)).astype(BF16)
    wide_q = jnp.dot(spread, q, preferred_element_type=F32)
    own_head = iota(wide_q.shape, 1) // HEAD == lax.rem(iota(wide_q.shape, 0), heads)
    qx[...] = jnp.where(own_head, wide_q, 0.0).astype(BF16)

    size = GROUP * heads
    row_of = iota((size, mine), 0)
    of_head = iota((size, mine), 1) // HEAD == lax.rem(row_of, heads)
    gather = (iota((CHUNK, CHUNK * heads), 1) // heads == iota((CHUNK, CHUNK * heads), 0)).astype(BF16)

    def attend(g, at):
        s = lax.rem(g, SLOTS)
        q16 = qx[pl.ds(pl.multiple_of(g * size, size), size), :].astype(F32)
        lhs = jnp.concatenate([jnp.where(row_of // heads == b, q16, 0.0).astype(BF16) for b in range(GROUP)], 1)
        take_k(g).wait()
        scores = jnp.dot(lhs, kbuf[s].reshape(GROUP * mine, cache), preferred_element_type=F32) * HEAD**-0.5
        e = jnp.exp(scores - jnp.max(scores, -1, keepdims=True))
        weights = (e * (1.0 / jnp.sum(e, -1, keepdims=True))).astype(BF16)
        take_v(g).wait()
        result = jnp.zeros((size, mine), F32)
        for b in range(GROUP):
            part = lax.dot_general(weights, vbuf[s, b], (((1,), (1,)), ((), ())), preferred_element_type=F32)
            result = jnp.where(row_of // heads == b, part, result)
        seen[pl.ds(pl.multiple_of(at * size, size), size), :] = jnp.where(of_head, result, 0.0).astype(BF16)

        @pl.when(g + SLOTS < groups)
        def _():
            take_k(g + SLOTS).start()
            take_v(g + SLOTS).start()

        for i, copy in enumerate((take_wg, take_wu, take_wd)):
            pl.when(g == groups - SLOTS + i)(copy.start)

    def reduce(c):
        all_arrived(rs_sem.at[c])
        finish(c, x, term, got, h)
        share(c, h, ag_sem)

    def chunk(c):
        each(per, lambda i: attend(c * per + i, i))
        now = jnp.dot(gather, seen[...], preferred_element_type=F32).astype(BF16)

        @pl.when(c == 0)
        def _():
            take_wo.wait()
            pl.semaphore_wait(barrier, n - 1)

        term[rows(c), :] = jnp.dot(now, wo[...], preferred_element_type=F32).astype(BF16)
        scatter(c, term, got, rs_sem)
        pl.when(c > 0)(lambda: reduce(c - 1))

    each(chunks, chunk)
    reduce(chunks - 1)

    def normed_again(c):
        all_arrived(ag_sem.at[c])
        norm(c, h, gain_m, a)

    each(chunks, normed_again)
    take_wg.wait()
    take_wu.wait()
    both = jnp.dot(a[...], wgu[...], preferred_element_type=F32)
    inner = (jax.nn.silu(both[:, :hidden]) * both[:, hidden:]).astype(BF16)
    take_wd.wait()
    term2[...] = jnp.dot(inner, wd[...], preferred_element_type=F32).astype(BF16)
    each(chunks, lambda c: scatter(c, term2, got2, rs2_sem))

    def reduce2(c):
        all_arrived(rs2_sem.at[c])
        finish(c, h, term2, got2, out)
        share(c, out, ag2_sem)

    each(chunks, reduce2)
    each(chunks, lambda c: all_arrived(ag2_sem.at[c]))
    each(4 * chunks, lambda c: all_arrived(send_sem))


def turns(place, heads):
    half = HEAD // 2
    angle = np.float32(place) * np.float32(THETA) ** (-np.arange(half, dtype=np.float32) / np.float32(half))
    cos, sin = np.cos(angle), np.sin(angle)
    return np.stack([np.tile(cos, 2 * heads), np.tile(np.concatenate([-sin, sin]), heads)]).astype(np.float32)


def solution(mesh):
    n = mesh.shape["tp"]

    def step(x, k_cache, v_cache, gain_a, wq, wo, gain_m, w_gate, w_up, w_down):
        batch, width = x.shape
        cache, heads = k_cache.shape[1:3]
        hidden = w_gate.shape[1]
        mine = heads * HEAD
        dims = batch, width, heads, cache, hidden

        def tall(t):
            return t.transpose(0, 2, 3, 1).reshape(batch, mine, cache)

        chunks = batch // CHUNK
        hbm, vmem = pl.BlockSpec(memory_space=pl.ANY), pl.BlockSpec(memory_space=pltpu.VMEM)
        got = pltpu.VMEM((chunks, n - 1, CHUNK, width // n), BF16)
        states = pltpu.VMEM((batch, width), BF16)
        dma = pltpu.SemaphoreType.DMA
        return pl.pallas_call(
            functools.partial(layer_kernel, n, dims),
            out_shape=jax.ShapeDtypeStruct(x.shape, BF16),
            in_specs=[hbm, hbm, hbm, vmem, hbm, hbm, vmem, hbm, hbm, hbm, vmem],
            out_specs=vmem,
            scratch_shapes=[
                states, states, pltpu.VMEM((width, mine), BF16), pltpu.VMEM((mine, width), BF16),
                pltpu.VMEM((width, 2 * hidden), BF16), pltpu.VMEM((hidden, width), BF16),
                pltpu.VMEM((SLOTS, GROUP, mine, cache), BF16), pltpu.VMEM((SLOTS, GROUP, mine, cache), BF16),
                pltpu.VMEM((batch * heads, mine), BF16), pltpu.VMEM((CHUNK * heads, mine), BF16),
                states, states, got, states, got,
                dma((6,)), dma((SLOTS,)), dma((SLOTS,)), dma, dma((chunks,)), dma((chunks,)), dma((chunks,)), dma((chunks,)),
            ],
            compiler_params=pltpu.CompilerParams(collective_id=0, has_side_effects=True, vmem_limit_bytes=63 * 2**20),
            name="layer",
        )(x, tall(k_cache), tall(v_cache), gain_a[None], wq, wo, gain_m[None], w_gate, w_up, w_down, turns(cache - 1, heads))

    states, cache, columns, rows_of = P("dp", None), P("dp", None, "tp", None), P(None, "tp"), P("tp", None)
    return jax.shard_map(
        step,
        mesh=mesh,
        in_specs=(states, cache, cache, P(None), columns, rows_of, P(None), columns, columns, rows_of),
        out_specs=states,
        check_vma=False,
    )
```

```python
import functools
import math

import jax
import jax.numpy as jnp
import numpy as np
from jax import lax
from jax.experimental import pallas as pl
from jax.experimental.pallas import tpu as pltpu
from jax.sharding import PartitionSpec as P

HEAD = 64
THETA = 10000
GROUP = 4
CHUNK = 16
SLOTS = 3

F32, BF16 = jnp.float32, jnp.bfloat16


def iota(shape, axis):
    return lax.broadcasted_iota(jnp.int32, shape, axis)


def layer_kernel(n, dims, x_hbm, k_hbm, v_hbm, ga_hbm, wq_hbm, wo_hbm, gm_hbm, wg_hbm, wu_hbm, wd_hbm, turn_hbm, out,
                 x, a, gain1, gain2, gains, turn, wq, wo, wgu, wd, kbuf, vbuf, weights, qx, seen, term, h, got, inner, term2, got2,
                 in_sem, k_sem, v_sem, send_sem, rs_sem, ag_sem, rs2_sem, ag2_sem):
    batch, width, heads, cache, hidden = dims
    mine = heads * HEAD
    cols = width // n
    chunks, groups = batch // CHUNK, batch // GROUP
    per = groups // chunks
    me = lax.axis_index("tp")

    def block(p):
        return pl.ds(pl.multiple_of(p * cols, cols), cols)

    def rows(c):
        return pl.ds(pl.multiple_of(c * CHUNK, CHUNK), CHUNK)

    side = math.isqrt(n)
    shape = (side, side) if side * side == n else (1, n)
    offsets = [(i, j) for i in range(shape[0]) for j in range(shape[1]) if i or j]
    offsets.sort(key=lambda o: -min(o[0], shape[0] - o[0]) - min(o[1], shape[1] - o[1]))

    def peer(k):
        i, j = offsets[k - 1]
        return lax.rem(me // shape[1] + i, shape[0]) * shape[1] + lax.rem(me + j, shape[1])

    def take(i, src, dst):
        return pltpu.make_async_copy(src, dst, in_sem.at[i])

    take_x, take_wq, take_wo = take(0, x_hbm, x), take(1, wq_hbm, wq), take(2, wo_hbm, wo)
    take_wg = take(3, wg_hbm, wgu.at[:, pl.ds(0, hidden)])
    take_wu = take(4, wu_hbm, wgu.at[:, pl.ds(hidden, hidden)])
    take_wd = take(5, wd_hbm, wd)
    small = take(6, ga_hbm, gain1), take(7, gm_hbm, gain2), take(8, turn_hbm, turn)

    def take_k(g):
        s = lax.rem(g, SLOTS)
        return pltpu.make_async_copy(k_hbm.at[pl.ds(g * GROUP, GROUP)], kbuf.at[s], k_sem.at[s])

    def take_v(g, b):
        s = lax.rem(g, SLOTS)
        return pltpu.make_async_copy(v_hbm.at[g * GROUP + b], vbuf.at[s, b], v_sem.at[s, b])

    def start_v(g):
        for b in range(GROUP):
            take_v(g, b).start()

    take_x.start()
    for copy in small:
        copy.start()
    take_wq.start()
    take_k(0).start()
    for g in range(SLOTS):
        if g + 1 < SLOTS:
            take_k(g + 1).start()
        start_v(g)
        if g == 0:
            take_wo.start()

    barrier = pltpu.get_barrier_semaphore()
    for k in range(1, n):
        pl.semaphore_signal(barrier, inc=1, device_id={"tp": peer(k)})

    def all_arrived(sem):
        pltpu.make_async_copy(got.at[0], got.at[0], sem).wait()

    def scatter(c, src, dst, sem):
        for k in range(1, n):
            pltpu.make_async_remote_copy(
                src_ref=src.at[rows(c), block(peer(k))],
                dst_ref=dst.at[c, k - 1],
                send_sem=send_sem,
                recv_sem=sem.at[c],
                device_id={"tp": peer(k)},
            ).start()

    def share(c, ref, sem):
        for k in range(1, n):
            pltpu.make_async_remote_copy(
                src_ref=ref.at[rows(c), block(me)],
                dst_ref=ref.at[rows(c), block(me)],
                send_sem=send_sem,
                recv_sem=sem.at[c],
                device_id={"tp": peer(k)},
            ).start()

    def finish(c, base, own, came, dst):
        total = base[rows(c), block(me)].astype(F32) + own[rows(c), block(me)].astype(F32)
        for k in range(n - 1):
            total += came[c, k].astype(F32)
        dst[rows(c), block(me)] = total.astype(BF16)

    def norm(c, src, i, dst):
        wide = src[rows(c), :].astype(F32)
        scale = lax.rsqrt(jnp.mean(wide * wide, -1, keepdims=True) + 1e-6)
        dst[rows(c), :] = (wide * scale * gains[i : i + 1, :]).astype(BF16)

    def each(count, body):
        lax.fori_loop(0, count, lambda i, _: (body(i), None)[1], None)

    for copy in small:
        copy.wait()
    for i, gain in enumerate((gain1, gain2)):
        gains[i : i + 1, :] = gain[...].astype(F32).reshape(1, width)
    take_x.wait()
    each(chunks, lambda c: norm(c, x, 0, a))
    take_wq.wait()
    q = jnp.dot(a[...], wq[...], preferred_element_type=F32).astype(BF16).astype(F32)
    low = lax.rem(iota(q.shape, 1), HEAD) < HEAD // 2
    other = jnp.where(low, pltpu.roll(q, mine - HEAD // 2, 1), pltpu.roll(q, HEAD // 2, 1))
    q = (q * turn[0:1, :] + other * turn[1:2, :]).astype(BF16)
    spread = (iota((batch * heads, batch), 0) // heads == iota((batch * heads, batch), 1)).astype(BF16)
    wide_q = jnp.dot(spread, q, preferred_element_type=F32)
    own_head = iota(wide_q.shape, 1) // HEAD == lax.rem(iota(wide_q.shape, 0), heads)
    qx[...] = jnp.where(own_head, wide_q, 0.0).astype(BF16)

    size = GROUP * heads
    row_of = iota((size, mine), 0)
    of_head = iota((size, mine), 1) // HEAD == lax.rem(row_of, heads)
    gather = (iota((CHUNK, CHUNK * heads), 1) // heads == iota((CHUNK, CHUNK * heads), 0)).astype(BF16)

    def weigh(g):
        q16 = qx[pl.ds(pl.multiple_of(g * size, size), size), :].astype(F32)
        lhs = jnp.concatenate([jnp.where(row_of // heads == b, q16, 0.0).astype(BF16) for b in range(GROUP)], 1)
        keys = kbuf[lax.rem(g, SLOTS)].reshape(GROUP * mine, cache)
        scores = jnp.dot(lhs, keys, preferred_element_type=F32) * HEAD**-0.5
        e = jnp.exp(scores - jnp.max(scores, -1, keepdims=True))
        return (e * (1.0 / jnp.sum(e, -1, keepdims=True))).astype(BF16)

    def value(g, b, result):
        part = lax.dot_general(weights[...], vbuf[lax.rem(g, SLOTS), b], (((1,), (1,)), ((), ())), preferred_element_type=F32)
        return jnp.where(row_of // heads == b, part, result)

    def keep(g, result):
        at = pl.ds(pl.multiple_of(lax.rem(g, per) * size, size), size)
        seen[at, :] = jnp.where(of_head, result, 0.0).astype(BF16)

    def attend(g):
        take_k(g + 1).wait()
        for b in range(GROUP):
            take_v(g, b).wait()
        result = jnp.zeros((size, mine), F32)
        for b in range(GROUP):
            result = value(g, b, result)
        later = weigh(g + 1)
        keep(g, result)
        weights[...] = later
        pl.when(g + 1 + SLOTS < groups)(lambda: take_k(g + 1 + SLOTS).start())
        pl.when(g + SLOTS < groups)(lambda: start_v(g + SLOTS))
        for i, copy in enumerate((take_wg, take_wu, take_wd)):
            pl.when(g == groups - SLOTS + min(i, SLOTS - 2))(copy.start)

    def reduce(c):
        all_arrived(rs_sem.at[c])
        finish(c, x, term, got, h)
        share(c, h, ag_sem)

    def send(c):
        now = jnp.dot(gather, seen[...], preferred_element_type=F32).astype(BF16)
        term[rows(c), :] = jnp.dot(now, wo[...], preferred_element_type=F32).astype(BF16)
        scatter(c, term, got, rs_sem)

    def step(g):
        c, i = g // per, lax.rem(g, per)
        pl.when((i == per // 2) & (c == 0))(lambda: pl.semaphore_wait(barrier, n - 1))
        pl.when((i == per // 2) & (c > 0))(lambda: reduce(c - 1))
        attend(g)
        pl.when(g == 0)(take_wo.wait)
        pl.when(i == per - 1)(lambda: send(c))

    def normed_again(c):
        all_arrived(ag_sem.at[c])
        norm(c, h, 1, a)

    def up(r):
        both = jnp.dot(a[r, :], wgu[...], preferred_element_type=F32)
        inner[r, :] = (jax.nn.silu(both[:, :hidden]) * both[:, hidden:]).astype(BF16)

    def down(r):
        term2[r, :] = jnp.dot(inner[r, :], wd[...], preferred_element_type=F32).astype(BF16)

    last = chunks - 1
    take_k(0).wait()
    weights[...] = weigh(0)
    take_k(SLOTS).start()
    each(groups - 1, step)
    result = jnp.zeros((size, mine), F32)
    for b in range(GROUP):
        take_v(groups - 1, b).wait()
        result = value(groups - 1, b, result)
    keep(groups - 1, result)
    send(last)
    early, late = slice(0, last * CHUNK), slice(last * CHUNK, batch)
    each(last, normed_again)
    take_wg.wait()
    take_wu.wait()
    up(early)
    reduce(last)
    take_wd.wait()
    down(early)
    each(last, lambda c: scatter(c, term2, got2, rs2_sem))
    normed_again(last)
    up(late)
    down(late)
    scatter(last, term2, got2, rs2_sem)

    def reduce2(c):
        all_arrived(rs2_sem.at[c])
        finish(c, h, term2, got2, out)
        share(c, out, ag2_sem)

    each(chunks, reduce2)
    each(chunks, lambda c: all_arrived(ag2_sem.at[c]))
    each(4 * chunks, lambda c: all_arrived(send_sem))


def turns(place, heads):
    half = HEAD // 2
    angle = np.float32(place) * np.float32(THETA) ** (-np.arange(half, dtype=np.float32) / np.float32(half))
    cos, sin = np.cos(angle), np.sin(angle)
    return np.stack([np.tile(cos, 2 * heads), np.tile(np.concatenate([-sin, sin]), heads)]).astype(np.float32)


def solution(mesh):
    n = mesh.shape["tp"]

    def step(x, k_cache, v_cache, gain_a, wq, wo, gain_m, w_gate, w_up, w_down):
        batch, width = x.shape
        cache, heads = k_cache.shape[1:3]
        hidden = w_gate.shape[1]
        mine = heads * HEAD
        dims = batch, width, heads, cache, hidden

        def tall(t):
            return t.transpose(0, 2, 3, 1).reshape(batch, mine, cache)

        chunks = batch // CHUNK
        hbm, vmem = pl.BlockSpec(memory_space=pltpu.HBM), pl.BlockSpec(memory_space=pltpu.VMEM)
        got = pltpu.VMEM((chunks, n - 1, CHUNK, width // n), BF16)
        states = pltpu.VMEM((batch, width), BF16)
        dma = pltpu.SemaphoreType.DMA
        return pl.pallas_call(
            functools.partial(layer_kernel, n, dims),
            out_shape=pltpu.VMEM(x.shape, BF16),
            in_specs=[hbm] * 11,
            out_specs=vmem,
            scratch_shapes=[
                states, states, pltpu.VMEM((width,), BF16), pltpu.VMEM((width,), BF16), pltpu.VMEM((2, width), F32), pltpu.VMEM((2, mine), F32),
                pltpu.VMEM((width, mine), BF16), pltpu.VMEM((mine, width), BF16),
                pltpu.VMEM((width, 2 * hidden), BF16), pltpu.VMEM((hidden, width), BF16),
                pltpu.VMEM((SLOTS, GROUP, mine, cache), BF16), pltpu.VMEM((SLOTS, GROUP, mine, cache), BF16),
                pltpu.VMEM((GROUP * heads, cache), BF16), pltpu.VMEM((batch * heads, mine), BF16), pltpu.VMEM((CHUNK * heads, mine), BF16),
                states, states, got, pltpu.VMEM((batch, hidden), BF16), states, got,
                dma((9,)), dma((SLOTS,)), dma((SLOTS, GROUP)), dma, dma((chunks,)), dma((chunks,)), dma((chunks,)), dma((chunks,)),
            ],
            compiler_params=pltpu.CompilerParams(collective_id=0, has_side_effects=True, vmem_limit_bytes=63 * 2**20),
            name="layer",
        )(x, tall(k_cache), tall(v_cache), gain_a, wq, wo, gain_m, w_gate, w_up, w_down, turns(cache - 1, heads))

    states, cache, columns, rows_of = P("dp", None), P("dp", None, "tp", None), P(None, "tp"), P("tp", None)
    return jax.shard_map(
        step,
        mesh=mesh,
        in_specs=(states, cache, cache, P(None), columns, rows_of, P(None), columns, columns, rows_of),
        out_specs=states,
        check_vma=False,
    )
```

```python
import functools
import math

import jax
import jax.numpy as jnp
import numpy as np
from jax import lax
from jax.experimental import pallas as pl
from jax.experimental.pallas import tpu as pltpu
from jax.sharding import PartitionSpec as P

HEAD = 64
THETA = 10000
GROUP = 4
CHUNK = 16
SLOTS = 3

F32, BF16 = jnp.float32, jnp.bfloat16


class Copies:
    def __init__(self, parts):
        self.parts = parts

    def start(self):
        for part in self.parts:
            part.start()

    def wait(self):
        for part in self.parts:
            part.wait()


def iota(shape, axis):
    return lax.broadcasted_iota(jnp.int32, shape, axis)


def layer_kernel(n, dims, x_hbm, k_hbm, v_hbm, ga_hbm, wq_hbm, wo_hbm, gm_hbm, wg_hbm, wu_hbm, wd_hbm, turn_hbm, out,
                 x, a, gain1, gain2, gains, turn, wq, wo, wgu, wd, kbuf, vbuf, weights, qx, seen, term, h, got, inner, term2, got2,
                 in_sem, k_sem, v_sem, send_sem, rs_sem, ag_sem, rs2_sem, ag2_sem):
    batch, width, heads, cache, hidden = dims
    mine = heads * HEAD
    cols = width // n
    chunks, groups = batch // CHUNK, batch // GROUP
    per = groups // chunks
    me = lax.axis_index("tp")

    def block(p):
        return pl.ds(pl.multiple_of(p * cols, cols), cols)

    def rows(c):
        return pl.ds(pl.multiple_of(c * CHUNK, CHUNK), CHUNK)

    side = math.isqrt(n)
    shape = (side, side) if side * side == n else (1, n)
    offsets = [(i, j) for i in range(shape[0]) for j in range(shape[1]) if i or j]
    offsets.sort(key=lambda o: -min(o[0], shape[0] - o[0]) - min(o[1], shape[1] - o[1]))

    def peer(k):
        i, j = offsets[k - 1]
        return lax.rem(me // shape[1] + i, shape[0]) * shape[1] + lax.rem(me + j, shape[1])

    def take(i, src, dst):
        return pltpu.make_async_copy(src, dst, in_sem.at[i])

    take_x, take_wq, take_wo = take(0, x_hbm, x), take(1, wq_hbm, wq), take(2, wo_hbm, wo)
    take_wg = take(3, wg_hbm, wgu.at[:, pl.ds(0, hidden)])
    take_wu = take(4, wu_hbm, wgu.at[:, pl.ds(hidden, hidden)])
    take_wd = take(5, wd_hbm, wd)
    small = take(6, ga_hbm, gain1), take(7, gm_hbm, gain2), take(8, turn_hbm, turn)

    def take_k(g):
        s = lax.rem(g, SLOTS)
        return Copies([pltpu.make_async_copy(k_hbm.at[g * GROUP + b], kbuf.at[s, b], k_sem.at[s, b]) for b in range(GROUP)])

    def take_v(g, b):
        s = lax.rem(g, SLOTS)
        return pltpu.make_async_copy(v_hbm.at[g * GROUP + b], vbuf.at[s, b], v_sem.at[s, b])

    def start_v(g):
        for b in range(GROUP):
            take_v(g, b).start()

    take_x.start()
    for copy in small:
        copy.start()
    take_wq.start()
    take_k(0).start()

    barrier = pltpu.get_barrier_semaphore()
    for k in range(1, n):
        pl.semaphore_signal(barrier, inc=1, device_id={"tp": peer(k)})

    def all_arrived(sem):
        pltpu.make_async_copy(got.at[0], got.at[0], sem).wait()

    def scatter(c, src, dst, sem):
        for k in range(1, n):
            pltpu.make_async_remote_copy(
                src_ref=src.at[rows(c), block(peer(k))],
                dst_ref=dst.at[c, k - 1],
                send_sem=send_sem,
                recv_sem=sem.at[c],
                device_id={"tp": peer(k)},
            ).start()

    def share(c, ref, sem):
        for k in range(1, n):
            pltpu.make_async_remote_copy(
                src_ref=ref.at[rows(c), block(me)],
                dst_ref=ref.at[rows(c), block(me)],
                send_sem=send_sem,
                recv_sem=sem.at[c],
                device_id={"tp": peer(k)},
            ).start()

    def finish(c, base, own, came, dst):
        total = base[rows(c), block(me)].astype(F32) + own[rows(c), block(me)].astype(F32)
        for k in range(n - 1):
            total += came[c, k].astype(F32)
        dst[rows(c), block(me)] = total.astype(BF16)

    def norm(c, src, i, dst):
        wide = src[rows(c), :].astype(F32)
        scale = lax.rsqrt(jnp.mean(wide * wide, -1, keepdims=True) + 1e-6)
        dst[rows(c), :] = (wide * scale * gains[i : i + 1, :]).astype(BF16)

    def each(count, body):
        lax.fori_loop(0, count, lambda i, _: (body(i), None)[1], None)

    for copy in small:
        copy.wait()
    for i, gain in enumerate((gain1, gain2)):
        gains[i : i + 1, :] = gain[...].astype(F32).reshape(1, width)
    take_x.wait()
    take_k(1).start()
    start_v(0)
    each(chunks, lambda c: norm(c, x, 0, a))
    take_wq.wait()
    take_wo.start()
    for g in range(1, SLOTS):
        if g + 1 < SLOTS:
            take_k(g + 1).start()
        start_v(g)
    q = jnp.dot(a[...], wq[...], preferred_element_type=F32).astype(BF16).astype(F32)
    low = lax.rem(iota(q.shape, 1), HEAD) < HEAD // 2
    other = jnp.where(low, pltpu.roll(q, mine - HEAD // 2, 1), pltpu.roll(q, HEAD // 2, 1))
    q = (q * turn[0:1, :] + other * turn[1:2, :]).astype(BF16)
    spread = (iota((batch * heads, batch), 0) // heads == iota((batch * heads, batch), 1)).astype(BF16)
    wide_q = jnp.dot(spread, q, preferred_element_type=F32)
    own_head = iota(wide_q.shape, 1) // HEAD == lax.rem(iota(wide_q.shape, 0), heads)
    qx[...] = jnp.where(own_head, wide_q, 0.0).astype(BF16)

    size = GROUP * heads
    row_of = iota((size, mine), 0)
    of_head = iota((size, mine), 1) // HEAD == lax.rem(row_of, heads)
    gather = (iota((CHUNK, CHUNK * heads), 1) // heads == iota((CHUNK, CHUNK * heads), 0)).astype(BF16)

    def weigh(g):
        q16 = qx[pl.ds(pl.multiple_of(g * size, size), size), :].astype(F32)
        lhs = jnp.concatenate([jnp.where(row_of // heads == b, q16, 0.0).astype(BF16) for b in range(GROUP)], 1)
        keys = kbuf[lax.rem(g, SLOTS)].reshape(GROUP * mine, cache)
        scores = jnp.dot(lhs, keys, preferred_element_type=F32) * HEAD**-0.5
        e = jnp.exp(scores - jnp.max(scores, -1, keepdims=True))
        return (e * (1.0 / jnp.sum(e, -1, keepdims=True))).astype(BF16)

    def value(g, b, result):
        part = lax.dot_general(weights[...], vbuf[lax.rem(g, SLOTS), b], (((1,), (1,)), ((), ())), preferred_element_type=F32)
        return jnp.where(row_of // heads == b, part, result)

    def keep(g, result):
        at = pl.ds(pl.multiple_of(lax.rem(g, per) * size, size), size)
        seen[at, :] = jnp.where(of_head, result, 0.0).astype(BF16)

    def attend(g):
        take_k(g + 1).wait()
        for b in range(GROUP):
            take_v(g, b).wait()
        result = jnp.zeros((size, mine), F32)
        for b in range(GROUP):
            result = value(g, b, result)
        later = weigh(g + 1)
        keep(g, result)
        weights[...] = later
        pl.when(g + 1 + SLOTS < groups)(lambda: take_k(g + 1 + SLOTS).start())
        pl.when(g + SLOTS < groups)(lambda: start_v(g + SLOTS))
        for i, copy in enumerate((take_wg, take_wu, take_wd)):
            pl.when(g == groups - SLOTS + min(i, SLOTS - 2))(copy.start)

    def reduce(c):
        all_arrived(rs_sem.at[c])
        finish(c, x, term, got, h)
        share(c, h, ag_sem)

    def send(c):
        now = jnp.dot(gather, seen[...], preferred_element_type=F32).astype(BF16)
        term[rows(c), :] = jnp.dot(now, wo[...], preferred_element_type=F32).astype(BF16)
        scatter(c, term, got, rs_sem)

    def step(g):
        c, i = g // per, lax.rem(g, per)
        pl.when((i == per // 2) & (c == 0))(lambda: pl.semaphore_wait(barrier, n - 1))
        pl.when((i == per // 2) & (c > 0))(lambda: reduce(c - 1))
        attend(g)
        pl.when(g == 0)(take_wo.wait)
        pl.when(i == per - 1)(lambda: send(c))

    def normed_again(c):
        all_arrived(ag_sem.at[c])
        norm(c, h, 1, a)

    def up(r):
        both = jnp.dot(a[r, :], wgu[...], preferred_element_type=F32)
        inner[r, :] = (jax.nn.silu(both[:, :hidden]) * both[:, hidden:]).astype(BF16)

    def down(r):
        term2[r, :] = jnp.dot(inner[r, :], wd[...], preferred_element_type=F32).astype(BF16)

    last = chunks - 1
    take_k(0).wait()
    weights[...] = weigh(0)
    take_k(SLOTS).start()
    each(groups - 1, step)
    result = jnp.zeros((size, mine), F32)
    for b in range(GROUP):
        take_v(groups - 1, b).wait()
        result = value(groups - 1, b, result)
    keep(groups - 1, result)
    send(last)
    early, late = slice(0, last * CHUNK), slice(last * CHUNK, batch)
    each(last, normed_again)
    take_wg.wait()
    take_wu.wait()
    up(early)
    reduce(last)
    take_wd.wait()
    down(early)
    each(last, lambda c: scatter(c, term2, got2, rs2_sem))
    normed_again(last)
    up(late)
    down(late)
    scatter(last, term2, got2, rs2_sem)

    def reduce2(c):
        all_arrived(rs2_sem.at[c])
        finish(c, h, term2, got2, out)
        share(c, out, ag2_sem)

    each(chunks, reduce2)
    each(chunks, lambda c: all_arrived(ag2_sem.at[c]))
    each(4 * chunks, lambda c: all_arrived(send_sem))


def turns(place, heads):
    half = HEAD // 2
    angle = np.float32(place) * np.float32(THETA) ** (-np.arange(half, dtype=np.float32) / np.float32(half))
    cos, sin = np.cos(angle), np.sin(angle)
    return np.stack([np.tile(cos, 2 * heads), np.tile(np.concatenate([-sin, sin]), heads)]).astype(np.float32)


def solution(mesh):
    n = mesh.shape["tp"]

    def step(x, k_cache, v_cache, gain_a, wq, wo, gain_m, w_gate, w_up, w_down):
        batch, width = x.shape
        cache, heads = k_cache.shape[1:3]
        hidden = w_gate.shape[1]
        mine = heads * HEAD
        dims = batch, width, heads, cache, hidden

        def tall(t):
            return t.transpose(0, 2, 3, 1).reshape(batch, mine, cache)

        chunks = batch // CHUNK
        hbm, vmem = pl.BlockSpec(memory_space=pltpu.HBM), pl.BlockSpec(memory_space=pltpu.VMEM)
        got = pltpu.VMEM((chunks, n - 1, CHUNK, width // n), BF16)
        states = pltpu.VMEM((batch, width), BF16)
        dma = pltpu.SemaphoreType.DMA
        return pl.pallas_call(
            functools.partial(layer_kernel, n, dims),
            out_shape=pltpu.VMEM(x.shape, BF16),
            in_specs=[hbm] * 11,
            out_specs=vmem,
            scratch_shapes=[
                states, states, pltpu.VMEM((width,), BF16), pltpu.VMEM((width,), BF16), pltpu.VMEM((2, width), F32), pltpu.VMEM((2, mine), F32),
                pltpu.VMEM((width, mine), BF16), pltpu.VMEM((mine, width), BF16),
                pltpu.VMEM((width, 2 * hidden), BF16), pltpu.VMEM((hidden, width), BF16),
                pltpu.VMEM((SLOTS, GROUP, mine, cache), BF16), pltpu.VMEM((SLOTS, GROUP, mine, cache), BF16),
                pltpu.VMEM((GROUP * heads, cache), BF16), pltpu.VMEM((batch * heads, mine), BF16), pltpu.VMEM((CHUNK * heads, mine), BF16),
                states, states, got, pltpu.VMEM((batch, hidden), BF16), states, got,
                dma((9,)), dma((SLOTS, GROUP)), dma((SLOTS, GROUP)), dma, dma((chunks,)), dma((chunks,)), dma((chunks,)), dma((chunks,)),
            ],
            compiler_params=pltpu.CompilerParams(collective_id=0, has_side_effects=True, vmem_limit_bytes=63 * 2**20),
            name="layer",
        )(x, tall(k_cache), tall(v_cache), gain_a, wq, wo, gain_m, w_gate, w_up, w_down, turns(cache - 1, heads))

    states, cache, columns, rows_of = P("dp", None), P("dp", None, "tp", None), P(None, "tp"), P("tp", None)
    return jax.shard_map(
        step,
        mesh=mesh,
        in_specs=(states, cache, cache, P(None), columns, rows_of, P(None), columns, columns, rows_of),
        out_specs=states,
        check_vma=False,
    )
```
